32 devices in a mesh: fsdp: 4 (over z), tp: 4 (over y, x), job: 2 (over core).
Axes of the slice: x: 2, y: 2, z: 4, core: 2. Of those that a mesh axis runs over, the one named last changes fastest.
Arguments:
- slopes_in: float32 [128, 128, 1024], P('job', 'fsdp', 'tp'), parts along dimension 0, may hold values from -6 to 6
- moments_in: float32 [128, 128, 1024], P('job', 'fsdp', 'tp'), parts along dimension 0, may hold values from -6 to 6
- weights_in: float32 [128, 128, 1024], P('job', 'fsdp', 'tp'), parts along dimension 0, may hold values from -0.1875 to 0.1875
Outputs:
- new_weights: float32 [128, 128, 1024], P('job', 'fsdp', 'tp'), parts along dimension 0
- new_momentum: float32 [128, 128, 1024], P('job', 'fsdp', 'tp'), parts along dimension 0
The draws below stay inside these ranges and needn't reach their ends.
There are 2 independent parts, one for each index of `job`. The reference program is written for one: setup_inputs(seed, part) draws one part's arguments, and reference() takes and returns one part's arrays. A program takes and returns all parts, laid end to end along the dimension named above; each array names one. Nothing has to cross between parts.
All inputs are finite; a program needn't handle non-finite values.
Results may differ from the reference program's by a relative error of at most 0.00019.
Values sent between devices are 32-bit elements; how exact they have to be, the bound alone decides.
A program may use at most 128 MiB of HBM per device.

```python
import jax
import jax.numpy as jnp
from jax import lax

SIDE = 128
WIDE = 1024
MATS = 64
ITERS = 5


def steps_of(stream_key, dims, shards, smallest, largest):
    def one(dim, parts):
        heights = jax.random.uniform(jax.random.fold_in(jax.random.fold_in(stream_key, 6), dim), (parts,), jnp.float32, smallest / len(shards), largest / len(shards))
        return jnp.repeat(jnp.exp(heights), dims[dim] // parts).reshape((-1,) + (1,) * (len(dims) - dim - 1))

    factor_of = one(*shards[0])
    for cut in shards[1:]:
        factor_of = factor_of * one(*cut)
    return factor_of


def scatter_about(own_key, extent, scale, bound, pieces=(), kind=jnp.bfloat16):
    drawn = jax.random.normal(own_key, extent, jnp.float32) * scale
    if len(pieces) > 0:
        drawn = steps_of(own_key, extent, pieces, -0.22, 0.18) * drawn
    return jnp.clip(drawn, min=-bound, max=bound).astype(kind)


def setup_inputs(seed: int = 0, part: int = 0) -> dict:
    arg_keys = jax.random.split(jax.random.key(seed), 4)
    part_splits = jax.random.split(jax.random.fold_in(arg_keys[3], part), 4)
    return {
        "slopes_in": scatter_about(part_splits[0], (MATS, SIDE, WIDE), 1.0, 6.0, ((1, 4), (2, 4)), jnp.float32),
        "moments_in": scatter_about(part_splits[1], (MATS, SIDE, WIDE), 1.0, 6.0, ((1, 4), (2, 4)), jnp.float32),
        "weights_in": scatter_about(part_splits[2], (MATS, SIDE, WIDE), 0.03, 0.1875, ((1, 4), (2, 4)), jnp.float32),
    }


hold_rate = 0.9
learn_rate = 0.8

def reference(slopes_in, moments_in, weights_in):
    new_momentum = hold_rate * moments_in + slopes_in

    def orthogonal_one(stack):
        iterate = stack[None]
        iterate = iterate * lax.rsqrt(lax.optimization_barrier(jnp.sum(iterate * iterate, axis=(1, 2), keepdims=True)) + 1e-06)
        for step in range(ITERS):
            gram = jnp.einsum('mik,mjk->mij', iterate, iterate, precision=lax.Precision.HIGHEST)
            mixed = -4.775 * gram + 2.0315 * jnp.einsum('mij,mjk->mik', gram, gram, precision=lax.Precision.HIGHEST)
            iterate = 3.4445 * iterate + jnp.einsum('mij,mjk->mik', mixed, iterate, precision=lax.Precision.HIGHEST)
        return iterate[0]
    iterate = lax.map(orthogonal_one, new_momentum)
    new_weights = weights_in - learn_rate * iterate
    return (new_weights, new_momentum)
```

```python
import functools

import jax
import jax.numpy as jnp
from jax import lax
from jax.experimental import pallas as pl
from jax.experimental.pallas import tpu as pltpu
from jax.sharding import PartitionSpec as P

ITERS = 5
LINE = 4


hold_rate = 0.9
learn_rate = 0.8

COEF_A, COEF_B, COEF_C = 3.4445, -4.775, 2.0315
MESH = pl.DeviceIdType.MESH
HIGHEST = lax.Precision.HIGHEST


def dot(a, b, contract=((1,), (0,))):
    return lax.dot_general(
        a, b, (contract, ((), ())), precision=HIGHEST, preferred_element_type=jnp.float32
    )


def factor_of(gram):
    side = gram.shape[0]
    rows = lax.broadcasted_iota(jnp.int32, (side, side), 0)
    eye = rows == lax.broadcasted_iota(jnp.int32, (side, side), 1)
    total = jnp.sum(jnp.where(eye, gram, 0.0), axis=(0, 1), keepdims=True)
    scale = lax.rsqrt(total + 1e-06)

    def mixed_of(a):
        return COEF_B * a + COEF_C * dot(a, a)

    def step(_, carry):
        a, q = carry
        mixed = mixed_of(a)
        half = COEF_A * a + dot(mixed, a)
        return COEF_A * half + dot(half, mixed), COEF_A * q + dot(mixed, q)

    a = gram * scale * scale
    q = jnp.where(eye, jnp.broadcast_to(scale, gram.shape), 0.0)
    a, q = lax.fori_loop(0, ITERS - 1, step, (a, q))
    return COEF_A * q + dot(mixed_of(a), q)


def kernel(nt, chunks, slopes, moments, weights, new, mom, out, wbuf, sbuf, mbuf, xbuf, gsend, grecv, qrecv, ybuf, sends, frecv, gr, qr, brecv, loads, hello, ready):
    me_f, me_t = lax.axis_index("fsdp"), lax.axis_index("tp")
    mats, rows, _ = mom.shape
    share = mats // LINE
    per = share // chunks
    each = per // nt

    half = me_f // 2
    far, near, side = 3 - 3 * half, 2 - half, me_f + 1 - 2 * lax.rem(me_f, 2)
    inner = me_f * (3 - me_f) > 0
    outer = me_f * (3 - me_f) == 0
    barrier = pltpu.get_barrier_semaphore()

    def tell(semaphore, device):
        pl.semaphore_signal(semaphore, inc=1, device_id=device, device_id_type=MESH)

    def tell_tp(semaphore):
        for d in range(1, nt):
            tell(semaphore, {"tp": lax.rem(me_t + d, nt)})

    @pl.when(inner)
    def _():
        tell(barrier, {"fsdp": near})

    @pl.when(outer)
    def _():
        tell_tp(barrier)

    order = [(c, peer) for c in range(chunks) for peer in (near, far, side, me_f)]

    def block(c, peer):
        return pl.ds(peer * share + c * per, per)

    def count(k):
        return k if k < 4 else 3 + k // 4

    def load(k):
        here = block(*order[k])
        return (
            pltpu.make_async_copy(slopes.at[here], sbuf.at[here], loads.at[count(k)]),
            pltpu.make_async_copy(moments.at[here], mbuf.at[here], loads.at[count(k)]),
        )

    for k in range(len(order)):
        for copy in load(k):
            copy.start()
    fetch = pltpu.make_async_copy(weights, wbuf, loads.at[count(len(order))])
    fetch.start()

    def loaded(k):
        if k < 4:
            some = pl.ds(0, 2 * per)
        elif k % 4 == 0:
            some = pl.ds(0, 8 * per)
        else:
            return
        pltpu.make_async_copy(slopes.at[some], sbuf.at[some], loads.at[count(k)]).wait()

    my_rows = pl.ds(pl.multiple_of(me_f * rows, rows), rows)

    def there(c, peer):
        return pltpu.make_async_remote_copy(
            src_ref=mom.at[block(c, peer)],
            dst_ref=xbuf.at[pl.ds(c * per, per), my_rows, :],
            send_sem=sends.at[0], recv_sem=frecv.at[c],
            device_id={"fsdp": peer}, device_id_type=MESH,
        )

    def back(c, peer):
        theirs = pl.ds(pl.multiple_of(peer * rows, rows), rows)
        return pltpu.make_async_remote_copy(
            src_ref=ybuf.at[pl.ds(c * per, per), theirs, :],
            dst_ref=out.at[block(c, me_f)],
            send_sem=sends.at[1], recv_sem=brecv.at[c],
            device_id={"fsdp": peer}, device_id_type=MESH,
        )

    def gram_copy(c, d):
        return pltpu.make_async_remote_copy(
            src_ref=gsend.at[c, d - 1], dst_ref=grecv.at[c, d],
            send_sem=sends.at[2], recv_sem=gr.at[c],
            device_id={"tp": lax.rem(me_t + d, nt)}, device_id_type=MESH,
        )

    def factor_copy(c, d):
        return pltpu.make_async_remote_copy(
            src_ref=qrecv.at[c, 0], dst_ref=qrecv.at[c, d],
            send_sem=sends.at[3], recv_sem=qr.at[c],
            device_id={"tp": lax.rem(me_t + d, nt)}, device_id_type=MESH,
        )

    def landed(ref, semaphore):
        pltpu.make_async_copy(ref, ref, semaphore).wait()

    def rows_landed(c, semaphores):
        landed(out.at[pl.ds(0, (LINE - 1) * per)], semaphores.at[c])

    def grams(c):
        rows_landed(c, frecv)
        for d in list(range(1, nt)) + [0]:
            first = c * per + lax.rem(me_t + d, nt) * each
            for e in range(each):
                x = xbuf[first + e]
                g = dot(x, x, ((1,), (1,)))
                if d == 0:
                    grecv[c, 0, e] = g
                else:
                    gsend[c, d - 1, e] = g
            if d > 0:
                gram_copy(c, d).start()

    def factors(c):
        landed(gsend.at[0], gr.at[c])
        for e in range(each):
            g = grecv[c, 0, e]
            for d in range(1, nt):
                g = g + grecv[c, d, e]
            qrecv[c, 0, e] = factor_of(g)
        for d in range(1, nt):
            factor_copy(c, d).start()

    def apply(c):
        for d in range(nt):
            if d == 1:
                landed(gsend.at[0], qr.at[c])
            first = c * per + lax.rem(me_t - d + nt, nt) * each
            for e in range(each):
                ybuf[first + e] = dot(qrecv[c, d, e], xbuf[first + e])
        for peer in (far, near, side):
            back(c, peer).start()
        out[block(c, me_f)] = ybuf[pl.ds(c * per, per), my_rows, :]

    def momentum(k):
        loaded(k)
        c, peer = order[k]
        here = block(c, peer)
        value = hold_rate * mbuf[here] + sbuf[here]
        mom[here] = value
        if k % 4 == 3:
            xbuf[pl.ds(c * per, per), my_rows, :] = value

    momentum(0)
    momentum(1)

    @pl.when(inner)
    def _():
        pl.semaphore_wait(barrier, 1)
        there(0, near).start()
        tell(barrier, {"fsdp": side})

    for k in range(2, len(order)):
        momentum(k)

    @pl.when(inner)
    def _():
        for c in range(1, min(chunks, 2)):
            there(c, near).start()
        pl.semaphore_wait(hello, 2)
        tell(hello, {"fsdp": side})
        for c in range(chunks):
            for peer in (near, far, side) if c > 1 else (far, side):
                there(c, peer).start()
        pl.semaphore_wait(ready, 1)

    @pl.when(outer)
    def _():
        pl.semaphore_wait(barrier, nt)
        tell(hello, {"fsdp": side})
        tell(hello, {"fsdp": near})
        for c in range(min(chunks, 2)):
            for peer in (near, side):
                there(c, peer).start()
        pl.semaphore_wait(hello, 1)
        for c in range(chunks):
            for peer in (near, far, side) if c > 1 else (far,):
                there(c, peer).start()
        tell_tp(ready)
        pl.semaphore_wait(ready, nt - 1)
        tell(ready, {"fsdp": side})

    grams(0)
    factors(0)
    apply(0)
    for c in range(1, chunks + 1):
        if c < chunks:
            grams(c)
        if c > 1:
            apply(c - 1)
        if c < chunks:
            factors(c)

    fetch.wait()
    for c in range(chunks):
        rows_landed(c, brecv)
        for peer in range(LINE):
            here = pl.ds(peer * share + c * per, per)
            new[here] = wbuf[here] - learn_rate * out[here]

    landed(mom.at[pl.ds(0, mats - share)], sends.at[0])
    landed(mom.at[pl.ds(0, mats - share)], sends.at[1])
    landed(gsend, sends.at[2])
    landed(gsend, sends.at[3])


def finish(new, mom, new_out, mom_out, sems):
    copies = []
    for k, (src, dst) in enumerate(((mom, mom_out), (new, new_out))):
        copies.append(pltpu.make_async_copy(src, dst, sems.at[k]))
    for copy in copies:
        copy.start()
    for copy in copies:
        copy.wait()


def stepped(nf, nt, slopes_in, moments_in, weights_in):
    mats, rows, wide = slopes_in.shape
    side, share = rows * nf, mats // nf
    most = share // nt
    chunks = max(k for k in range(1, 5) if most % k == 0)
    per = share // chunks
    each = per // nt
    vmem, dma, flag = pltpu.VMEM, pltpu.SemaphoreType.DMA, pltpu.SemaphoreType.REGULAR
    shape = jax.ShapeDtypeStruct(slopes_in.shape, jnp.float32)
    held = [pl.BlockSpec(memory_space=pltpu.VMEM)] * 2
    far = [pl.BlockSpec(memory_space=pltpu.HBM)]
    results = pl.pallas_call(
        functools.partial(kernel, nt, chunks),
        out_shape=[shape] * 2,
        in_specs=far * 3,
        out_specs=held,
        scratch_shapes=[
            vmem(slopes_in.shape, jnp.float32),
            vmem(slopes_in.shape, jnp.float32),
            vmem(slopes_in.shape, jnp.float32),
            vmem(slopes_in.shape, jnp.float32),
            vmem((share, side, wide), jnp.float32),
            vmem((chunks, nt - 1, each, side, side), jnp.float32),
            vmem((chunks, nt, each, side, side), jnp.float32),
            vmem((chunks, nt, each, side, side), jnp.float32),
            vmem((share, side, wide), jnp.float32),
            dma((4,)), dma((chunks,)), dma((chunks,)), dma((chunks,)), dma((chunks,)),
            dma((4 + chunks,)), flag, flag,
        ],
        compiler_params=pltpu.CompilerParams(
            collective_id=0, has_side_effects=True, vmem_limit_bytes=32 * 2**20
        ),
    )(*(pltpu.with_memory_space_constraint(x, pltpu.HBM) for x in (slopes_in, moments_in, weights_in)))
    return pl.pallas_call(
        finish,
        out_shape=[shape] * 2,
        in_specs=held,
        out_specs=far * 2,
        scratch_shapes=[dma((2,))],
        compiler_params=pltpu.CompilerParams(vmem_limit_bytes=2**20),
    )(*results)


def orthogonal_plain(new_momentum):
    moved = lax.all_to_all(new_momentum, "fsdp", split_axis=0, concat_axis=1, tiled=True)
    gram = lax.dot_general(moved, moved, (((2,), (2,)), ((0,), (0,))), precision=HIGHEST)
    gram = lax.psum_scatter(gram, "tp", scatter_dimension=0, tiled=True)
    factors = lax.all_gather(jax.vmap(factor_of)(gram), "tp", axis=0, tiled=True)
    whole = lax.dot_general(factors, moved, (((2,), (1,)), ((0,), (0,))), precision=HIGHEST)
    return lax.all_to_all(whole, "fsdp", split_axis=1, concat_axis=0, tiled=True)


def body(nf, nt, slopes_in, moments_in, weights_in):
    rows, wide = slopes_in.shape[1:]
    if nf == LINE and nt > 1 and rows % 8 == 0 and wide % 128 == 0:
        return stepped(nf, nt, slopes_in, moments_in, weights_in)
    new_momentum = hold_rate * moments_in + slopes_in
    new_weights = weights_in - learn_rate * orthogonal_plain(new_momentum)
    return (new_weights, new_momentum)


def solution(mesh):
    placed = (P("job", "fsdp", "tp"), P("job", "fsdp", "tp"), P("job", "fsdp", "tp"))
    return jax.shard_map(
        functools.partial(body, mesh.shape["fsdp"], mesh.shape["tp"]),
        mesh=mesh,
        in_specs=placed,
        out_specs=(P("job", "fsdp", "tp"), P("job", "fsdp", "tp")),
        check_vma=False,
    )
```

```python
import functools

import jax
import jax.numpy as jnp
from jax import lax
from jax.experimental import pallas as pl
from jax.experimental.pallas import tpu as pltpu
from jax.sharding import PartitionSpec as P

ITERS = 5
LINE = 4
AHEAD = 2


hold_rate = 0.9
learn_rate = 0.8

COEF_A, COEF_B, COEF_C = 3.4445, -4.775, 2.0315
MESH = pl.DeviceIdType.MESH
HIGHEST = lax.Precision.HIGHEST


def dot(a, b, contract=((1,), (0,))):
    return lax.dot_general(
        a, b, (contract, ((), ())), precision=HIGHEST, preferred_element_type=jnp.float32
    )


def factor_of(gram):
    side = gram.shape[0]
    rows = lax.broadcasted_iota(jnp.int32, (side, side), 0)
    eye = rows == lax.broadcasted_iota(jnp.int32, (side, side), 1)
    total = jnp.sum(jnp.where(eye, gram, 0.0), axis=(0, 1), keepdims=True)
    scale = lax.rsqrt(total + 1e-06)

    def mixed_of(a):
        return COEF_B * a + COEF_C * dot(a, a)

    def step(_, carry):
        a, q = carry
        mixed = mixed_of(a)
        half = COEF_A * a + dot(mixed, a)
        return COEF_A * half + dot(half, mixed), COEF_A * q + dot(mixed, q)

    a = gram * scale * scale
    q = jnp.where(eye, jnp.broadcast_to(scale, gram.shape), 0.0)
    a, q = lax.fori_loop(0, ITERS - 1, step, (a, q))
    return COEF_A * q + dot(mixed_of(a), q)


def kernel(nt, chunks, slopes, moments, weights, early, new, mom, out, wbuf, inputs, xbuf, gsend, grecv, qrecv, ybuf, sends, frecv, gr, qr, brecv, loads, hello, ready):
    me_f, me_t = lax.axis_index("fsdp"), lax.axis_index("tp")
    mats, rows, _ = mom.shape
    share = mats // LINE
    per = share // chunks
    each = per // nt

    half = me_f // 2
    far, near, side = 3 - 3 * half, 2 - half, me_f + 1 - 2 * lax.rem(me_f, 2)
    inner = me_f * (3 - me_f) > 0
    outer = me_f * (3 - me_f) == 0
    barrier = pltpu.get_barrier_semaphore()

    def tell(semaphore, device):
        pl.semaphore_signal(semaphore, inc=1, device_id=device, device_id_type=MESH)

    def tell_tp(semaphore):
        for d in range(1, nt):
            tell(semaphore, {"tp": lax.rem(me_t + d, nt)})

    @pl.when(inner)
    def _():
        tell(barrier, {"fsdp": near})

    @pl.when(outer)
    def _():
        tell_tp(barrier)

    order = [(c, peer) for c in range(chunks) for peer in (near, far, side, me_f)]

    def block(c, peer):
        return pl.ds(peer * share + c * per, per)

    groups = [(0, 1), (1, LINE), (LINE, 2 * LINE), (2 * LINE, chunks * LINE)]

    def request(group):
        for k in range(*groups[group]):
            here = block(*order[k])
            pltpu.make_async_copy(slopes.at[here], inputs.at[0, here], loads.at[group]).start()
            pltpu.make_async_copy(moments.at[here], inputs.at[1, here], loads.at[group]).start()

    def landed(ref, semaphore):
        pltpu.make_async_copy(ref, ref, semaphore).wait()

    request(0)
    fetch = pltpu.make_async_copy(weights, wbuf, loads.at[len(groups)])

    my_rows = pl.ds(pl.multiple_of(me_f * rows, rows), rows)

    def there(c, peer):
        return pltpu.make_async_remote_copy(
            src_ref=mom.at[block(c, peer)],
            dst_ref=xbuf.at[pl.ds(c * per, per), my_rows, :],
            send_sem=sends.at[0], recv_sem=frecv.at[c],
            device_id={"fsdp": peer}, device_id_type=MESH,
        )

    def back(c, peer):
        theirs = pl.ds(pl.multiple_of(peer * rows, rows), rows)
        return pltpu.make_async_remote_copy(
            src_ref=ybuf.at[pl.ds(c * per, per), theirs, :],
            dst_ref=out.at[block(c, me_f)],
            send_sem=sends.at[1], recv_sem=brecv.at[c],
            device_id={"fsdp": peer}, device_id_type=MESH,
        )

    def gram_copy(c, d):
        return pltpu.make_async_remote_copy(
            src_ref=gsend.at[c, d - 1], dst_ref=grecv.at[c, d],
            send_sem=sends.at[2], recv_sem=gr.at[c],
            device_id={"tp": lax.rem(me_t + d, nt)}, device_id_type=MESH,
        )

    def factor_copy(c, d):
        return pltpu.make_async_remote_copy(
            src_ref=qrecv.at[c, 0], dst_ref=qrecv.at[c, d],
            send_sem=sends.at[3], recv_sem=qr.at[c],
            device_id={"tp": lax.rem(me_t + d, nt)}, device_id_type=MESH,
        )

    def rows_landed(c, semaphores):
        landed(out.at[pl.ds(0, (LINE - 1) * per)], semaphores.at[c])

    def grams(c):
        rows_landed(c, frecv)
        for d in list(range(1, nt)) + [0]:
            first = c * per + lax.rem(me_t + d, nt) * each
            for e in range(each):
                x = xbuf[first + e]
                g = dot(x, x, ((1,), (1,)))
                if d == 0:
                    grecv[c, 0, e] = g
                else:
                    gsend[c, d - 1, e] = g
            if d > 0:
                gram_copy(c, d).start()

    def factors(c):
        landed(gsend.at[0], gr.at[c])
        for e in range(each):
            g = grecv[c, 0, e]
            for d in range(1, nt):
                g = g + grecv[c, d, e]
            qrecv[c, 0, e] = factor_of(g)
        for d in range(1, nt):
            factor_copy(c, d).start()

    def apply(c):
        for d in range(nt):
            if d == 1:
                landed(gsend.at[0], qr.at[c])
            first = c * per + lax.rem(me_t - d + nt, nt) * each
            for e in range(each):
                ybuf[first + e] = dot(qrecv[c, d, e], xbuf[first + e])
        for peer in (far, near, side):
            back(c, peer).start()
        out[block(c, me_f)] = ybuf[pl.ds(c * per, per), my_rows, :]

    def momentum(group):
        first, last = groups[group]
        if last > first:
            landed(inputs.at[:, pl.ds(0, (last - first) * per)], loads.at[group])
        for k in range(first, last):
            c, peer = order[k]
            here = block(c, peer)
            value = hold_rate * inputs[1, here] + inputs[0, here]
            mom[here] = value
            if k % LINE == LINE - 1:
                xbuf[pl.ds(c * per, per), my_rows, :] = value

    momentum(0)
    request(1)

    @pl.when(inner)
    def _():
        pl.semaphore_wait(barrier, 1)
        there(0, near).start()
        tell(barrier, {"fsdp": side})

    request(2)
    request(3)
    fetch.start()
    for group in range(1, len(groups)):
        momentum(group)

    @pl.when(inner)
    def _():
        for c in range(1, min(chunks, AHEAD)):
            there(c, near).start()
        pl.semaphore_wait(hello, 2)
        tell(hello, {"fsdp": side})
        for c in range(chunks):
            for peer in (near, far, side) if c >= AHEAD else (far, side):
                there(c, peer).start()
        pl.semaphore_wait(ready, 1)

    @pl.when(outer)
    def _():
        pl.semaphore_wait(barrier, nt)
        tell(hello, {"fsdp": side})
        tell(hello, {"fsdp": near})
        for c in range(min(chunks, AHEAD)):
            for peer in (near, side):
                there(c, peer).start()
        pl.semaphore_wait(hello, 1)
        for c in range(chunks):
            for peer in (near, far, side) if c >= AHEAD else (far,):
                there(c, peer).start()
        tell_tp(ready)
        pl.semaphore_wait(ready, nt - 1)
        tell(ready, {"fsdp": side})

    grams(0)
    factors(0)
    apply(0)
    for c in range(1, chunks + 1):
        if c < chunks:
            grams(c)
        if c > 1:
            apply(c - 1)
        if c < chunks:
            factors(c)

    fetch.wait()
    for c in range(chunks):
        rows_landed(c, brecv)
        for peer in range(LINE):
            here = pl.ds(peer * share + c * per, per)
            new[here] = wbuf[here] - learn_rate * out[here]

    landed(mom.at[pl.ds(0, mats - share)], sends.at[0])
    landed(mom.at[pl.ds(0, mats - share)], sends.at[1])
    landed(gsend, sends.at[2])
    landed(gsend, sends.at[3])


def early_momentum(slopes, moments, mom_out, inputs, held, loads, writes):
    @pl.when(lax.axis_index("fsdp") == 0)
    def _():
        parts = loads.shape[0]
        some = mom_out.shape[0] // parts

        def part(j):
            return pl.ds(j * some, some)

        for j in range(parts):
            pltpu.make_async_copy(slopes.at[part(j)], inputs.at[0, part(j)], loads.at[j]).start()
            pltpu.make_async_copy(moments.at[part(j)], inputs.at[1, part(j)], loads.at[j]).start()
        for j in range(parts):
            arrived = inputs.at[:, part(j)]
            pltpu.make_async_copy(arrived, arrived, loads.at[j]).wait()
            held[part(j)] = hold_rate * inputs[1, part(j)] + inputs[0, part(j)]
            pltpu.make_async_copy(held.at[part(j)], mom_out.at[part(j)], writes).start()
        pltpu.make_async_copy(held, mom_out, writes).wait()


def finish(new, mom, early, new_out, mom_out, sems):
    late = lax.axis_index("fsdp") > 0
    rest = pltpu.make_async_copy(mom, mom_out, sems.at[0])
    pl.when(late)(rest.start)
    last = pltpu.make_async_copy(new, new_out, sems.at[1])
    last.start()
    pl.when(late)(rest.wait)
    last.wait()


def stepped(nf, nt, slopes_in, moments_in, weights_in):
    mats, rows, wide = slopes_in.shape
    side, share = rows * nf, mats // nf
    most = share // nt
    chunks = max(k for k in range(1, 5) if most % k == 0)
    per = share // chunks
    each = per // nt
    vmem, dma, flag = pltpu.VMEM, pltpu.SemaphoreType.DMA, pltpu.SemaphoreType.REGULAR
    shape = jax.ShapeDtypeStruct(slopes_in.shape, jnp.float32)
    held = [pl.BlockSpec(memory_space=pltpu.VMEM)] * 2
    far = [pl.BlockSpec(memory_space=pltpu.HBM)]
    inputs = [pltpu.with_memory_space_constraint(x, pltpu.HBM) for x in (slopes_in, moments_in, weights_in)]
    early = pl.pallas_call(
        early_momentum,
        out_shape=shape,
        in_specs=far * 2,
        out_specs=far[0],
        scratch_shapes=[
            vmem((2,) + slopes_in.shape, jnp.float32),
            vmem(slopes_in.shape, jnp.float32),
            dma((max(k for k in range(1, 5) if mats % k == 0),)), dma,
        ],
        compiler_params=pltpu.CompilerParams(vmem_limit_bytes=16 * 2**20),
    )(*inputs[:2])
    early = pltpu.with_memory_space_constraint(early, pltpu.HBM)
    new, mom = pl.pallas_call(
        functools.partial(kernel, nt, chunks),
        out_shape=[shape] * 2,
        in_specs=far * 4,
        out_specs=held,
        scratch_shapes=[
            vmem(slopes_in.shape, jnp.float32),
            vmem(slopes_in.shape, jnp.float32),
            vmem((2,) + slopes_in.shape, jnp.float32),
            vmem((share, side, wide), jnp.float32),
            vmem((chunks, nt - 1, each, side, side), jnp.float32),
            vmem((chunks, nt, each, side, side), jnp.float32),
            vmem((chunks, nt, each, side, side), jnp.float32),
            vmem((share, side, wide), jnp.float32),
            dma((4,)), dma((chunks,)), dma((chunks,)), dma((chunks,)), dma((chunks,)),
            dma((5,)), flag, flag,
        ],
        compiler_params=pltpu.CompilerParams(
            collective_id=0, has_side_effects=True, vmem_limit_bytes=32 * 2**20
        ),
    )(*inputs, early)
    return pl.pallas_call(
        finish,
        out_shape=[shape] * 2,
        in_specs=held + far,
        out_specs=far * 2,
        input_output_aliases={2: 1},
        scratch_shapes=[dma((2,))],
        compiler_params=pltpu.CompilerParams(vmem_limit_bytes=2**20),
    )(new, mom, early)


def orthogonal_plain(new_momentum):
    moved = lax.all_to_all(new_momentum, "fsdp", split_axis=0, concat_axis=1, tiled=True)
    gram = lax.dot_general(moved, moved, (((2,), (2,)), ((0,), (0,))), precision=HIGHEST)
    gram = lax.psum_scatter(gram, "tp", scatter_dimension=0, tiled=True)
    factors = lax.all_gather(jax.vmap(factor_of)(gram), "tp", axis=0, tiled=True)
    whole = lax.dot_general(factors, moved, (((2,), (1,)), ((0,), (0,))), precision=HIGHEST)
    return lax.all_to_all(whole, "fsdp", split_axis=1, concat_axis=0, tiled=True)


def body(nf, nt, slopes_in, moments_in, weights_in):
    rows, wide = slopes_in.shape[1:]
    if nf == LINE and nt > 1 and rows % 8 == 0 and wide % 128 == 0:
        return stepped(nf, nt, slopes_in, moments_in, weights_in)
    new_momentum = hold_rate * moments_in + slopes_in
    new_weights = weights_in - learn_rate * orthogonal_plain(new_momentum)
    return (new_weights, new_momentum)


def solution(mesh):
    placed = (P("job", "fsdp", "tp"), P("job", "fsdp", "tp"), P("job", "fsdp", "tp"))
    return jax.shard_map(
        functools.partial(body, mesh.shape["fsdp"], mesh.shape["tp"]),
        mesh=mesh,
        in_specs=placed,
        out_specs=(P("job", "fsdp", "tp"), P("job", "fsdp", "tp")),
        check_vma=False,
    )
```

```python
import functools

import jax
import jax.numpy as jnp
from jax import lax
from jax.experimental import pallas as pl
from jax.experimental.pallas import tpu as pltpu
from jax.sharding import PartitionSpec as P

ITERS = 5
LINE = 4
AHEAD = 2
LATE_CHUNKS = (1, 2)
CHUNKS = 4
ORDER = ((0, 0), (1, 0), (2, 0), (0, 1), (1, 1), (0, 2), (2, 1), (1, 2), (0, 3), (1, 3), (2, 2), (2, 3))


hold_rate = 0.9
learn_rate = 0.8

COEF_A, COEF_B, COEF_C = 3.4445, -4.775, 2.0315
MESH = pl.DeviceIdType.MESH
HIGHEST = lax.Precision.HIGHEST


def dot(a, b, contract=((1,), (0,))):
    return lax.dot_general(
        a, b, (contract, ((), ())), precision=HIGHEST, preferred_element_type=jnp.float32
    )


def factor_of(gram):
    side = gram.shape[0]
    rows = lax.broadcasted_iota(jnp.int32, (side, side), 0)
    eye = rows == lax.broadcasted_iota(jnp.int32, (side, side), 1)
    total = jnp.sum(jnp.where(eye, gram, 0.0), axis=(0, 1), keepdims=True)
    scale = lax.rsqrt(total + 1e-06)

    def mixed_of(a):
        return COEF_B * a + COEF_C * dot(a, a)

    def step(_, carry):
        a, q = carry
        mixed = mixed_of(a)
        half = COEF_A * a + dot(mixed, a)
        return COEF_A * half + dot(half, mixed), COEF_A * q + dot(mixed, q)

    a = gram * scale * scale
    q = jnp.where(eye, jnp.broadcast_to(scale, gram.shape), 0.0)
    a, q = lax.fori_loop(0, ITERS - 1, step, (a, q))
    return COEF_A * q + dot(mixed_of(a), q)


def places():
    me_f = lax.axis_index("fsdp")
    half = me_f // 2
    return me_f, 3 - 3 * half, 2 - half, me_f + 1 - 2 * lax.rem(me_f, 2)


def tell(semaphore, device):
    pl.semaphore_signal(semaphore, inc=1, device_id=device, device_id_type=MESH)


def landed(ref, semaphore):
    pltpu.make_async_copy(ref, ref, semaphore).wait()


def pieces_of(share, chunks):
    per = share // chunks
    return [(c * per, per) for c in range(chunks)]


def each_job(pieces, act):
    kind = lax.rem(lax.axis_index("job"), 2)
    for number, late in enumerate(LATE_CHUNKS):
        pl.when(kind == number)(functools.partial(act, len(pieces) - late))


def back_copy(ybuf, out, sends, arrivals, share, me_f, peer, piece):
    start, size = piece
    rows = out.shape[1]
    theirs = pl.ds(pl.multiple_of(peer * rows, rows), rows)
    return pltpu.make_async_remote_copy(
        src_ref=ybuf.at[pl.ds(start, size), theirs, :],
        dst_ref=out.at[pl.ds(me_f * share + start, size)],
        send_sem=sends, recv_sem=arrivals,
        device_id={"fsdp": peer}, device_id_type=MESH,
    )


def own_rows(ybuf, out, share, me_f, piece):
    start, size = piece
    rows = out.shape[1]
    mine = pl.ds(pl.multiple_of(me_f * rows, rows), rows)
    out[pl.ds(me_f * share + start, size)] = ybuf[pl.ds(start, size), mine, :]


def update(new, wbuf, out, arrivals, share, piece):
    start, size = piece
    landed(out.at[pl.ds(0, (LINE - 1) * size)], arrivals)
    for owner in range(LINE):
        here = pl.ds(owner * share + start, size)
        new[here] = wbuf[here] - learn_rate * out[here]


def sent(out, sends, pieces):
    total = sum(size for _, size in pieces)
    landed(out.at[pl.ds(0, (LINE - 1) * total)], sends)


def kernel(nt, chunks, slopes, moments, weights, new, mom, ybuf, wbuf, out, inputs, xbuf, gsend, grecv, qrecv, sends, frecv, gr, qr, brecv, loads, hello, ready):
    me_f, far, near, side = places()
    me_t = lax.axis_index("tp")
    mats, rows, _ = mom.shape
    share = mats // LINE
    per = share // chunks
    each = per // nt
    pieces = pieces_of(share, chunks)

    inner = me_f * (3 - me_f) > 0
    outer = me_f * (3 - me_f) == 0
    barrier = pltpu.get_barrier_semaphore()

    def tell_tp(semaphore):
        for d in range(1, nt):
            tell(semaphore, {"tp": lax.rem(me_t + d, nt)})

    @pl.when(inner)
    def _():
        tell(barrier, {"fsdp": near})

    @pl.when(outer)
    def _():
        tell_tp(barrier)

    order = [(c, peer) for c in range(chunks) for peer in (near, far, side, me_f)]

    def block(c, peer):
        return pl.ds(peer * share + c * per, per)

    groups = [(0, 1), (1, LINE), (LINE, 2 * LINE), (2 * LINE, chunks * LINE)]

    def request(group):
        for k in range(*groups[group]):
            here = block(*order[k])
            pltpu.make_async_copy(slopes.at[here], inputs.at[0, here], loads.at[group]).start()
            pltpu.make_async_copy(moments.at[here], inputs.at[1, here], loads.at[group]).start()

    request(0)
    fetch = pltpu.make_async_copy(weights, wbuf, loads.at[len(groups)])

    my_rows = pl.ds(pl.multiple_of(me_f * rows, rows), rows)

    def there(c, peer):
        return pltpu.make_async_remote_copy(
            src_ref=mom.at[block(c, peer)],
            dst_ref=xbuf.at[pl.ds(c * per, per), my_rows, :],
            send_sem=sends.at[0], recv_sem=frecv.at[c],
            device_id={"fsdp": peer}, device_id_type=MESH,
        )

    def gram_copy(c, d):
        return pltpu.make_async_remote_copy(
            src_ref=gsend.at[c, d - 1], dst_ref=grecv.at[c, d],
            send_sem=sends.at[2], recv_sem=gr.at[c],
            device_id={"tp": lax.rem(me_t + d, nt)}, device_id_type=MESH,
        )

    def factor_copy(c, d):
        return pltpu.make_async_remote_copy(
            src_ref=qrecv.at[c, 0], dst_ref=qrecv.at[c, d],
            send_sem=sends.at[3], recv_sem=qr.at[c],
            device_id={"tp": lax.rem(me_t + d, nt)}, device_id_type=MESH,
        )

    def grams(c):
        landed(out.at[pl.ds(0, (LINE - 1) * per)], frecv.at[c])
        for d in list(range(1, nt)) + [0]:
            first = c * per + lax.rem(me_t + d, nt) * each
            for e in range(each):
                x = xbuf[first + e]
                g = dot(x, x, ((1,), (1,)))
                if d == 0:
                    grecv[c, 0, e] = g
                else:
                    gsend[c, d - 1, e] = g
            if d > 0:
                gram_copy(c, d).start()

    def factors(c):
        landed(gsend.at[0], gr.at[c])
        for e in range(each):
            g = grecv[c, 0, e]
            for d in range(1, nt):
                g = g + grecv[c, d, e]
            qrecv[c, 0, e] = factor_of(g)
        for d in range(1, nt):
            factor_copy(c, d).start()

    def apply(c):
        for d in range(nt):
            if d == 1:
                landed(gsend.at[0], qr.at[c])
            first = c * per + lax.rem(me_t - d + nt, nt) * each
            for e in range(each):
                ybuf[first + e] = dot(qrecv[c, d, e], xbuf[first + e])

        def give(late):
            for k, piece in enumerate(pieces[:late]):
                if c * per <= piece[0] < (c + 1) * per:
                    for peer in (far, near, side):
                        back_copy(ybuf, out, sends.at[1], brecv.at[k], share, me_f, peer, piece).start()

        each_job(pieces, give)
        own_rows(ybuf, out, share, me_f, (c * per, per))

    def momentum(group):
        first, last = groups[group]
        if last > first:
            landed(inputs.at[:, pl.ds(0, (last - first) * per)], loads.at[group])
        for k in range(first, last):
            c, peer = order[k]
            here = block(c, peer)
            value = hold_rate * inputs[1, here] + inputs[0, here]
            mom[here] = value
            if k % LINE == LINE - 1:
                xbuf[pl.ds(c * per, per), my_rows, :] = value

    momentum(0)
    request(1)

    @pl.when(inner)
    def _():
        pl.semaphore_wait(barrier, 1)
        there(0, near).start()
        tell(barrier, {"fsdp": side})

    request(2)
    request(3)
    fetch.start()
    for group in range(1, len(groups)):
        momentum(group)

    @pl.when(inner)
    def _():
        for c in range(1, min(chunks, AHEAD)):
            there(c, near).start()
        pl.semaphore_wait(hello, 2)
        tell(hello, {"fsdp": side})
        for c in range(chunks):
            for peer in (near, far, side) if c >= AHEAD else (far, side):
                there(c, peer).start()
        pl.semaphore_wait(ready, 1)

    @pl.when(outer)
    def _():
        pl.semaphore_wait(barrier, nt)
        tell(hello, {"fsdp": side})
        tell(hello, {"fsdp": near})
        for c in range(min(chunks, AHEAD)):
            for peer in (near, side):
                there(c, peer).start()
        pl.semaphore_wait(hello, 1)
        for c in range(chunks):
            for peer in (near, far, side) if c >= AHEAD else (far,):
                there(c, peer).start()
        tell_tp(ready)
        pl.semaphore_wait(ready, nt - 1)
        tell(ready, {"fsdp": side})

    for act, c in ORDER:
        (grams, factors, apply)[act](c)

    fetch.wait()

    def take(late):
        for k, piece in enumerate(pieces[:late]):
            update(new, wbuf, out, brecv.at[k], share, piece)
        sent(out, sends.at[1], pieces[:late])

    each_job(pieces, take)
    landed(mom.at[pl.ds(0, mats - share)], sends.at[0])
    landed(gsend, sends.at[2])
    landed(gsend, sends.at[3])


def last_kernel(chunks, ybuf, wbuf, written, new, out, sends, arrivals):
    me_f, far, near, side = places()
    share = ybuf.shape[0]
    pieces = pieces_of(share, chunks)
    barrier = pltpu.get_barrier_semaphore()
    for peer in (near, far, side):
        tell(barrier, {"fsdp": peer})

    def finish_job(late):
        pl.semaphore_wait(barrier, LINE - 1)
        for peer in (far, near, side):
            for k, piece in enumerate(pieces[late:]):
                back_copy(ybuf, out, sends, arrivals.at[k], share, me_f, peer, piece).start()
        for piece in pieces[late:]:
            own_rows(ybuf, out, share, me_f, piece)
        for k, piece in enumerate(pieces[late:]):
            update(new, wbuf, out, arrivals.at[k], share, piece)
        sent(out, sends, pieces[late:])

    each_job(pieces, finish_job)


def copies_of(new, new_out, sems, share, first, last):
    copies = []
    for owner in range(LINE):
        here = pl.ds(owner * share + first, last - first)
        copies.append(pltpu.make_async_copy(new.at[here], new_out.at[here], sems.at[owner]))
    return copies


def write_first(chunks, new, mom, new_out, mom_out, sems):
    share = new.shape[0] // LINE
    pieces = pieces_of(share, chunks)

    def write(late):
        copies = [pltpu.make_async_copy(mom, mom_out, sems.at[LINE])]
        copies += copies_of(new, new_out, sems, share, 0, pieces[late][0])
        for copy in copies:
            copy.start()
        for copy in copies:
            copy.wait()

    each_job(pieces, write)


def write_last(chunks, new, written, new_out, sems):
    share = new.shape[0] // LINE
    pieces = pieces_of(share, chunks)

    def write(late):
        copies = copies_of(new, new_out, sems, share, pieces[late][0], share)
        for copy in copies:
            copy.start()
        for copy in copies:
            copy.wait()

    each_job(pieces, write)


def stepped(nf, nt, slopes_in, moments_in, weights_in):
    mats, rows, wide = slopes_in.shape
    side, share = rows * nf, mats // nf
    chunks = CHUNKS
    per = share // chunks
    each = per // nt
    vmem, dma, flag = pltpu.VMEM, pltpu.SemaphoreType.DMA, pltpu.SemaphoreType.REGULAR
    shape = jax.ShapeDtypeStruct(slopes_in.shape, jnp.float32)
    whole = jax.ShapeDtypeStruct((share, side, wide), jnp.float32)
    held = [pl.BlockSpec(memory_space=pltpu.VMEM)]
    far = [pl.BlockSpec(memory_space=pltpu.HBM)]
    new, mom, results, weights = pl.pallas_call(
        functools.partial(kernel, nt, chunks),
        out_shape=[shape, shape, whole, shape],
        in_specs=far * 3,
        out_specs=held * 4,
        scratch_shapes=[
            vmem(slopes_in.shape, jnp.float32),
            vmem((2,) + slopes_in.shape, jnp.float32),
            vmem((share, side, wide), jnp.float32),
            vmem((chunks, nt - 1, each, side, side), jnp.float32),
            vmem((chunks, nt, each, side, side), jnp.float32),
            vmem((chunks, nt, each, side, side), jnp.float32),
            dma((4,)), dma((chunks,)), dma((chunks,)), dma((chunks,)), dma((chunks,)),
            dma((5,)), flag, flag,
        ],
        compiler_params=pltpu.CompilerParams(
            collective_id=0, has_side_effects=True, vmem_limit_bytes=32 * 2**20
        ),
    )(*(pltpu.with_memory_space_constraint(x, pltpu.HBM) for x in (slopes_in, moments_in, weights_in)))
    new_out, mom_out = pl.pallas_call(
        functools.partial(write_first, chunks),
        out_shape=[shape] * 2,
        in_specs=held * 2,
        out_specs=far * 2,
        scratch_shapes=[dma((LINE + 1,))],
        compiler_params=pltpu.CompilerParams(vmem_limit_bytes=2**20),
    )(new, mom)
    new_out = pltpu.with_memory_space_constraint(new_out, pltpu.HBM)
    last = pl.pallas_call(
        functools.partial(last_kernel, chunks),
        out_shape=shape,
        in_specs=held * 2 + far,
        out_specs=held[0],
        scratch_shapes=[vmem(slopes_in.shape, jnp.float32), dma, dma((max(LATE_CHUNKS),))],
        compiler_params=pltpu.CompilerParams(
            collective_id=1, has_side_effects=True, vmem_limit_bytes=4 * 2**20
        ),
    )(results, weights, new_out)
    new_out = pl.pallas_call(
        functools.partial(write_last, chunks),
        out_shape=shape,
        in_specs=held + far,
        out_specs=far[0],
        input_output_aliases={1: 0},
        scratch_shapes=[dma((LINE,))],
        compiler_params=pltpu.CompilerParams(vmem_limit_bytes=2**20),
    )(last, new_out)
    return new_out, mom_out


def orthogonal_plain(new_momentum):
    moved = lax.all_to_all(new_momentum, "fsdp", split_axis=0, concat_axis=1, tiled=True)
    gram = lax.dot_general(moved, moved, (((2,), (2,)), ((0,), (0,))), precision=HIGHEST)
    gram = lax.psum_scatter(gram, "tp", scatter_dimension=0, tiled=True)
    factors = lax.all_gather(jax.vmap(factor_of)(gram), "tp", axis=0, tiled=True)
    whole = lax.dot_general(factors, moved, (((2,), (1,)), ((0,), (0,))), precision=HIGHEST)
    return lax.all_to_all(whole, "fsdp", split_axis=1, concat_axis=0, tiled=True)


def body(nf, nt, slopes_in, moments_in, weights_in):
    rows, wide = slopes_in.shape[1:]
    share = slopes_in.shape[0] // nf
    if nf == LINE and nt > 1 and share % (CHUNKS * nt) == 0 and rows % 8 == 0 and wide % 128 == 0:
        return stepped(nf, nt, slopes_in, moments_in, weights_in)
    new_momentum = hold_rate * moments_in + slopes_in
    new_weights = weights_in - learn_rate * orthogonal_plain(new_momentum)
    return (new_weights, new_momentum)


def solution(mesh):
    placed = (P("job", "fsdp", "tp"), P("job", "fsdp", "tp"), P("job", "fsdp", "tp"))
    return jax.shard_map(
        functools.partial(body, mesh.shape["fsdp"], mesh.shape["tp"]),
        mesh=mesh,
        in_specs=placed,
        out_specs=(P("job", "fsdp", "tp"), P("job", "fsdp", "tp")),
        check_vma=False,
    )
```

```python
import functools

import jax
import jax.numpy as jnp
from jax import lax
from jax.experimental import pallas as pl
from jax.experimental.pallas import tpu as pltpu
from jax.sharding import PartitionSpec as P

ITERS = 5
LINE = 4
AHEAD = 2
LATE_CHUNKS = (0, 2)
CHUNKS = 4
ORDER = ((0, 0), (1, 0), (2, 0), (0, 1), (1, 1), (0, 2), (2, 1), (1, 2), (0, 3), (1, 3), (2, 2), (2, 3))


hold_rate = 0.9
learn_rate = 0.8

COEF_A, COEF_B, COEF_C = 3.4445, -4.775, 2.0315
MESH = pl.DeviceIdType.MESH
HIGHEST = lax.Precision.HIGHEST


def dot(a, b, contract=((1,), (0,))):
    return lax.dot_general(
        a, b, (contract, ((), ())), precision=HIGHEST, preferred_element_type=jnp.float32
    )


def factor_of(gram):
    side = gram.shape[0]
    rows = lax.broadcasted_iota(jnp.int32, (side, side), 0)
    eye = rows == lax.broadcasted_iota(jnp.int32, (side, side), 1)
    total = jnp.sum(jnp.where(eye, gram, 0.0), axis=(0, 1), keepdims=True)
    scale = lax.rsqrt(total + 1e-06)

    def mixed_of(a):
        return COEF_B * a + COEF_C * dot(a, a)

    def step(_, carry):
        a, q = carry
        mixed = mixed_of(a)
        half = COEF_A * a + dot(mixed, a)
        return COEF_A * half + dot(half, mixed), COEF_A * q + dot(mixed, q)

    a = gram * scale * scale
    q = jnp.where(eye, jnp.broadcast_to(scale, gram.shape), 0.0)
    a, q = lax.fori_loop(0, ITERS - 1, step, (a, q))
    return COEF_A * q + dot(mixed_of(a), q)


def places():
    me_f = lax.axis_index("fsdp")
    half = me_f // 2
    return me_f, 3 - 3 * half, 2 - half, me_f + 1 - 2 * lax.rem(me_f, 2)


def tell(semaphore, device):
    pl.semaphore_signal(semaphore, inc=1, device_id=device, device_id_type=MESH)


def landed(ref, semaphore):
    pltpu.make_async_copy(ref, ref, semaphore).wait()


def pieces_of(share, chunks):
    per = share // chunks
    return [(c * per, per) for c in range(chunks)]


def each_job(pieces, act):
    kind = lax.rem(lax.axis_index("job"), 2)
    for number, late in enumerate(LATE_CHUNKS):
        pl.when(kind == number)(functools.partial(act, len(pieces) - late))


def back_copy(ybuf, out, sends, arrivals, share, me_f, peer, piece):
    start, size = piece
    rows = out.shape[1]
    theirs = pl.ds(pl.multiple_of(peer * rows, rows), rows)
    return pltpu.make_async_remote_copy(
        src_ref=ybuf.at[pl.ds(start, size), theirs, :],
        dst_ref=out.at[pl.ds(me_f * share + start, size)],
        send_sem=sends, recv_sem=arrivals,
        device_id={"fsdp": peer}, device_id_type=MESH,
    )


def own_rows(ybuf, out, share, me_f, piece):
    start, size = piece
    rows = out.shape[1]
    mine = pl.ds(pl.multiple_of(me_f * rows, rows), rows)
    out[pl.ds(me_f * share + start, size)] = ybuf[pl.ds(start, size), mine, :]


def update(new, wbuf, out, arrivals, share, piece):
    start, size = piece
    landed(out.at[pl.ds(0, (LINE - 1) * size)], arrivals)
    for owner in range(LINE):
        here = pl.ds(owner * share + start, size)
        new[here] = wbuf[here] - learn_rate * out[here]


def sent(out, sends, pieces):
    total = sum(size for _, size in pieces)
    landed(out.at[pl.ds(0, (LINE - 1) * total)], sends)


def kernel(nt, chunks, slopes, moments, weights, new, mom, ybuf, wbuf, out, inputs, xbuf, gsend, grecv, qrecv, sends, frecv, gr, qr, brecv, loads, hello, ready):
    me_f, far, near, side = places()
    me_t = lax.axis_index("tp")
    mats, rows, _ = mom.shape
    share = mats // LINE
    per = share // chunks
    each = per // nt
    pieces = pieces_of(share, chunks)

    inner = me_f * (3 - me_f) > 0
    outer = me_f * (3 - me_f) == 0
    barrier = pltpu.get_barrier_semaphore()

    def tell_tp(semaphore):
        for d in range(1, nt):
            tell(semaphore, {"tp": lax.rem(me_t + d, nt)})

    @pl.when(inner)
    def _():
        tell(barrier, {"fsdp": near})

    @pl.when(outer)
    def _():
        tell_tp(barrier)

    order = [(c, peer) for c in range(chunks) for peer in (near, far, side, me_f)]

    def block(c, peer):
        return pl.ds(peer * share + c * per, per)

    groups = [(0, 1), (1, LINE), (LINE, 2 * LINE), (2 * LINE, chunks * LINE)]

    def request(group):
        for k in range(*groups[group]):
            here = block(*order[k])
            pltpu.make_async_copy(slopes.at[here], inputs.at[0, here], loads.at[group]).start()
            pltpu.make_async_copy(moments.at[here], inputs.at[1, here], loads.at[group]).start()

    request(0)
    fetch = pltpu.make_async_copy(weights, wbuf, loads.at[len(groups)])

    my_rows = pl.ds(pl.multiple_of(me_f * rows, rows), rows)

    def there(c, peer):
        return pltpu.make_async_remote_copy(
            src_ref=mom.at[block(c, peer)],
            dst_ref=xbuf.at[pl.ds(c * per, per), my_rows, :],
            send_sem=sends.at[0], recv_sem=frecv.at[c],
            device_id={"fsdp": peer}, device_id_type=MESH,
        )

    def gram_copy(c, d):
        return pltpu.make_async_remote_copy(
            src_ref=gsend.at[c, d - 1], dst_ref=grecv.at[c, d],
            send_sem=sends.at[2], recv_sem=gr.at[c],
            device_id={"tp": lax.rem(me_t + d, nt)}, device_id_type=MESH,
        )

    def factor_copy(c, d):
        return pltpu.make_async_remote_copy(
            src_ref=qrecv.at[c, 0], dst_ref=qrecv.at[c, d],
            send_sem=sends.at[3], recv_sem=qr.at[c],
            device_id={"tp": lax.rem(me_t + d, nt)}, device_id_type=MESH,
        )

    def grams(c):
        landed(out.at[pl.ds(0, (LINE - 1) * per)], frecv.at[c])
        for d in list(range(1, nt)) + [0]:
            first = c * per + lax.rem(me_t + d, nt) * each
            for e in range(each):
                x = xbuf[first + e]
                g = dot(x, x, ((1,), (1,)))
                if d == 0:
                    grecv[c, 0, e] = g
                else:
                    gsend[c, d - 1, e] = g
            if d > 0:
                gram_copy(c, d).start()

    def factors(c):
        landed(gsend.at[0], gr.at[c])
        for e in range(each):
            g = grecv[c, 0, e]
            for d in range(1, nt):
                g = g + grecv[c, d, e]
            qrecv[c, 0, e] = factor_of(g)
        for d in range(1, nt):
            factor_copy(c, d).start()

    def apply(c):
        for d in range(nt):
            if d == 1:
                landed(gsend.at[0], qr.at[c])
            first = c * per + lax.rem(me_t - d + nt, nt) * each
            for e in range(each):
                ybuf[first + e] = dot(qrecv[c, d, e], xbuf[first + e])

        def give(late):
            for k, piece in enumerate(pieces[:late]):
                if c * per <= piece[0] < (c + 1) * per:
                    for peer in (far, near, side):
                        back_copy(ybuf, out, sends.at[1], brecv.at[k], share, me_f, peer, piece).start()

        each_job(pieces, give)
        own_rows(ybuf, out, share, me_f, (c * per, per))

    def momentum(group):
        first, last = groups[group]
        if last > first:
            landed(inputs.at[:, pl.ds(0, (last - first) * per)], loads.at[group])
        for k in range(first, last):
            c, peer = order[k]
            here = block(c, peer)
            value = hold_rate * inputs[1, here] + inputs[0, here]
            mom[here] = value
            if k % LINE == LINE - 1:
                xbuf[pl.ds(c * per, per), my_rows, :] = value

    momentum(0)
    request(1)

    @pl.when(inner)
    def _():
        pl.semaphore_wait(barrier, 1)
        there(0, near).start()
        tell(barrier, {"fsdp": side})

    request(2)
    request(3)
    fetch.start()
    for group in range(1, len(groups)):
        momentum(group)

    @pl.when(inner)
    def _():
        for c in range(1, min(chunks, AHEAD)):
            there(c, near).start()
        pl.semaphore_wait(hello, 2)
        tell(hello, {"fsdp": side})
        for c in range(chunks):
            for peer in (near, far, side) if c >= AHEAD else (far, side):
                there(c, peer).start()
        pl.semaphore_wait(ready, 1)

    @pl.when(outer)
    def _():
        pl.semaphore_wait(barrier, nt)
        tell(hello, {"fsdp": side})
        tell(hello, {"fsdp": near})
        for c in range(min(chunks, AHEAD)):
            for peer in (near, side):
                there(c, peer).start()
        pl.semaphore_wait(hello, 1)
        for c in range(chunks):
            for peer in (near, far, side) if c >= AHEAD else (far,):
                there(c, peer).start()
        tell_tp(ready)
        pl.semaphore_wait(ready, nt - 1)
        tell(ready, {"fsdp": side})

    for act, c in ORDER:
        (grams, factors, apply)[act](c)

    fetch.wait()

    def take(late):
        for k, piece in enumerate(pieces[:late]):
            update(new, wbuf, out, brecv.at[k], share, piece)
        sent(out, sends.at[1], pieces[:late])

    each_job(pieces, take)
    landed(mom.at[pl.ds(0, mats - share)], sends.at[0])
    landed(gsend, sends.at[2])
    landed(gsend, sends.at[3])


def last_kernel(chunks, ybuf, wbuf, written, new, out, sends, arrivals):
    me_f, far, near, side = places()
    share = ybuf.shape[0]
    pieces = pieces_of(share, chunks)
    barrier = pltpu.get_barrier_semaphore()

    def finish_job(late):
        if late == len(pieces):
            return
        for peer in (near, far, side):
            tell(barrier, {"fsdp": peer})
        pl.semaphore_wait(barrier, LINE - 1)
        for peer in (far, near, side):
            for k, piece in enumerate(pieces[late:]):
                back_copy(ybuf, out, sends, arrivals.at[k], share, me_f, peer, piece).start()
        for piece in pieces[late:]:
            own_rows(ybuf, out, share, me_f, piece)
        for k, piece in enumerate(pieces[late:]):
            update(new, wbuf, out, arrivals.at[k], share, piece)
        sent(out, sends, pieces[late:])

    each_job(pieces, finish_job)


def copies_of(new, new_out, sems, share, pieces):
    copies = []
    for owner in range(LINE if pieces else 0):
        here = pl.ds(owner * share + pieces[0][0], sum(size for _, size in pieces))
        copies.append(pltpu.make_async_copy(new.at[here], new_out.at[here], sems.at[owner]))
    return copies


def write_first(chunks, new, mom, new_out, mom_out, sems):
    share = new.shape[0] // LINE
    pieces = pieces_of(share, chunks)

    def write(late):
        copies = [pltpu.make_async_copy(mom, mom_out, sems.at[LINE])]
        copies += copies_of(new, new_out, sems, share, pieces[:late])
        for copy in copies:
            copy.start()
        for copy in copies:
            copy.wait()

    each_job(pieces, write)


def write_last(chunks, new, written, new_out, sems):
    share = new.shape[0] // LINE
    pieces = pieces_of(share, chunks)

    def write(late):
        copies = copies_of(new, new_out, sems, share, pieces[late:])
        for copy in copies:
            copy.start()
        for copy in copies:
            copy.wait()

    each_job(pieces, write)


def stepped(nf, nt, slopes_in, moments_in, weights_in):
    mats, rows, wide = slopes_in.shape
    side, share = rows * nf, mats // nf
    chunks = CHUNKS
    per = share // chunks
    each = per // nt
    vmem, dma, flag = pltpu.VMEM, pltpu.SemaphoreType.DMA, pltpu.SemaphoreType.REGULAR
    shape = jax.ShapeDtypeStruct(slopes_in.shape, jnp.float32)
    whole = jax.ShapeDtypeStruct((share, side, wide), jnp.float32)
    held = [pl.BlockSpec(memory_space=pltpu.VMEM)]
    far = [pl.BlockSpec(memory_space=pltpu.HBM)]
    new, mom, results, weights = pl.pallas_call(
        functools.partial(kernel, nt, chunks),
        out_shape=[shape, shape, whole, shape],
        in_specs=far * 3,
        out_specs=held * 4,
        scratch_shapes=[
            vmem(slopes_in.shape, jnp.float32),
            vmem((2,) + slopes_in.shape, jnp.float32),
            vmem((share, side, wide), jnp.float32),
            vmem((chunks, nt - 1, each, side, side), jnp.float32),
            vmem((chunks, nt, each, side, side), jnp.float32),
            vmem((chunks, nt, each, side, side), jnp.float32),
            dma((4,)), dma((chunks,)), dma((chunks,)), dma((chunks,)), dma((chunks,)),
            dma((5,)), flag, flag,
        ],
        compiler_params=pltpu.CompilerParams(
            collective_id=0, has_side_effects=True, vmem_limit_bytes=32 * 2**20
        ),
    )(*(pltpu.with_memory_space_constraint(x, pltpu.HBM) for x in (slopes_in, moments_in, weights_in)))
    new_out, mom_out = pl.pallas_call(
        functools.partial(write_first, chunks),
        out_shape=[shape] * 2,
        in_specs=held * 2,
        out_specs=far * 2,
        scratch_shapes=[dma((LINE + 1,))],
        compiler_params=pltpu.CompilerParams(vmem_limit_bytes=2**20),
    )(new, mom)
    new_out = pltpu.with_memory_space_constraint(new_out, pltpu.HBM)
    last = pl.pallas_call(
        functools.partial(last_kernel, chunks),
        out_shape=shape,
        in_specs=held * 2 + far,
        out_specs=held[0],
        scratch_shapes=[vmem(slopes_in.shape, jnp.float32), dma, dma((max(LATE_CHUNKS),))],
        compiler_params=pltpu.CompilerParams(
            collective_id=1, has_side_effects=True, vmem_limit_bytes=4 * 2**20
        ),
    )(results, weights, new_out)
    new_out = pl.pallas_call(
        functools.partial(write_last, chunks),
        out_shape=shape,
        in_specs=held + far,
        out_specs=far[0],
        input_output_aliases={1: 0},
        scratch_shapes=[dma((LINE,))],
        compiler_params=pltpu.CompilerParams(vmem_limit_bytes=2**20),
    )(last, new_out)
    return new_out, mom_out


def orthogonal_plain(new_momentum):
    moved = lax.all_to_all(new_momentum, "fsdp", split_axis=0, concat_axis=1, tiled=True)
    gram = lax.dot_general(moved, moved, (((2,), (2,)), ((0,), (0,))), precision=HIGHEST)
    gram = lax.psum_scatter(gram, "tp", scatter_dimension=0, tiled=True)
    factors = lax.all_gather(jax.vmap(factor_of)(gram), "tp", axis=0, tiled=True)
    whole = lax.dot_general(factors, moved, (((2,), (1,)), ((0,), (0,))), precision=HIGHEST)
    return lax.all_to_all(whole, "fsdp", split_axis=1, concat_axis=0, tiled=True)


def body(nf, nt, slopes_in, moments_in, weights_in):
    rows, wide = slopes_in.shape[1:]
    share = slopes_in.shape[0] // nf
    if nf == LINE and nt > 1 and share % (CHUNKS * nt) == 0 and rows % 8 == 0 and wide % 128 == 0:
        return stepped(nf, nt, slopes_in, moments_in, weights_in)
    new_momentum = hold_rate * moments_in + slopes_in
    new_weights = weights_in - learn_rate * orthogonal_plain(new_momentum)
    return (new_weights, new_momentum)


def solution(mesh):
    placed = (P("job", "fsdp", "tp"), P("job", "fsdp", "tp"), P("job", "fsdp", "tp"))
    return jax.shard_map(
        functools.partial(body, mesh.shape["fsdp"], mesh.shape["tp"]),
        mesh=mesh,
        in_specs=placed,
        out_specs=(P("job", "fsdp", "tp"), P("job", "fsdp", "tp")),
        check_vma=False,
    )
```

```python
import functools

import jax
import jax.numpy as jnp
from jax import lax
from jax.experimental import pallas as pl
from jax.experimental.pallas import tpu as pltpu
from jax.sharding import PartitionSpec as P

ITERS = 5
LINE = 4
AHEAD = 2
LATE_PIECES = ((0, 0), (2, 2))
CHUNKS = 4
ORDER = ((0, 0), (1, 0), (2, 0), (0, 1), (1, 1), (0, 2), (2, 1), (1, 2), (0, 3), (1, 3), (2, 2), (2, 3))


hold_rate = 0.9
learn_rate = 0.8

COEF_A, COEF_B, COEF_C = 3.4445, -4.775, 2.0315
MESH = pl.DeviceIdType.MESH
HIGHEST = lax.Precision.HIGHEST


def dot(a, b, contract=((1,), (0,))):
    return lax.dot_general(
        a, b, (contract, ((), ())), precision=HIGHEST, preferred_element_type=jnp.float32
    )


def factor_of(gram):
    side = gram.shape[0]
    rows = lax.broadcasted_iota(jnp.int32, (side, side), 0)
    eye = rows == lax.broadcasted_iota(jnp.int32, (side, side), 1)
    total = jnp.sum(jnp.where(eye, gram, 0.0), axis=(0, 1), keepdims=True)
    scale = lax.rsqrt(total + 1e-06)

    def mixed_of(a):
        return COEF_B * a + COEF_C * dot(a, a)

    def step(_, carry):
        a, q = carry
        mixed = mixed_of(a)
        half = COEF_A * a + dot(mixed, a)
        return COEF_A * half + dot(half, mixed), COEF_A * q + dot(mixed, q)

    a = gram * scale * scale
    q = jnp.where(eye, jnp.broadcast_to(scale, gram.shape), 0.0)
    a, q = lax.fori_loop(0, ITERS - 1, step, (a, q))
    return COEF_A * q + dot(mixed_of(a), q)


def places():
    me_f = lax.axis_index("fsdp")
    half = me_f // 2
    return me_f, 3 - 3 * half, 2 - half, me_f + 1 - 2 * lax.rem(me_f, 2)


def tell(semaphore, device):
    pl.semaphore_signal(semaphore, inc=1, device_id=device, device_id_type=MESH)


def landed(ref, semaphore):
    pltpu.make_async_copy(ref, ref, semaphore).wait()


def pieces_of(share, chunks):
    per = share // chunks
    first = share - 2 * per
    whole = [(c * per, per) for c in range(chunks)]
    return whole[:-2] + [(first, per // 2), (first + per // 2, per - per // 2)] + whole[-1:]


def each_job(pieces, act):
    kind = lax.rem(lax.axis_index("job"), 2)
    me_f = lax.axis_index("fsdp")
    place = me_f * (3 - me_f)
    for number, late in enumerate(LATE_PIECES):
        ends, inside = (len(pieces) - few for few in late)
        if ends == inside:
            pl.when(kind == number)(functools.partial(act, ends, ends, ends, ends))
        else:
            pl.when((kind == number) & (place > 0))(functools.partial(act, ends, inside, ends, inside))
            pl.when((kind == number) & (place == 0))(functools.partial(act, ends, inside, inside, ends))


def back_copy(ybuf, out, sends, arrivals, share, me_f, peer, piece):
    start, size = piece
    rows = out.shape[1]
    theirs = pl.ds(pl.multiple_of(peer * rows, rows), rows)
    return pltpu.make_async_remote_copy(
        src_ref=ybuf.at[pl.ds(start, size), theirs, :],
        dst_ref=out.at[pl.ds(me_f * share + start, size)],
        send_sem=sends, recv_sem=arrivals,
        device_id={"fsdp": peer}, device_id_type=MESH,
    )


def own_rows(ybuf, out, share, me_f, piece):
    start, size = piece
    rows = out.shape[1]
    mine = pl.ds(pl.multiple_of(me_f * rows, rows), rows)
    out[pl.ds(me_f * share + start, size)] = ybuf[pl.ds(start, size), mine, :]


def update(new, wbuf, out, arrivals, share, piece):
    start, size = piece
    landed(out.at[pl.ds(0, (LINE - 1) * size)], arrivals)
    for owner in range(LINE):
        here = pl.ds(owner * share + start, size)
        new[here] = wbuf[here] - learn_rate * out[here]


def sent(out, sends, groups):
    total = sum(size for pieces in groups for _, size in pieces)
    landed(out.at[pl.ds(0, total)], sends)


def kernel(nt, chunks, slopes, moments, weights, new, mom, ybuf, wbuf, out, inputs, xbuf, gsend, grecv, qrecv, sends, frecv, gr, qr, brecv, loads, hello, ready):
    me_f, far, near, side = places()
    me_t = lax.axis_index("tp")
    mats, rows, _ = mom.shape
    share = mats // LINE
    per = share // chunks
    each = per // nt
    pieces = pieces_of(share, chunks)

    inner = me_f * (3 - me_f) > 0
    outer = me_f * (3 - me_f) == 0
    barrier = pltpu.get_barrier_semaphore()

    def tell_tp(semaphore):
        for d in range(1, nt):
            tell(semaphore, {"tp": lax.rem(me_t + d, nt)})

    @pl.when(inner)
    def _():
        tell(barrier, {"fsdp": near})

    @pl.when(outer)
    def _():
        tell_tp(barrier)

    order = [(c, peer) for c in range(chunks) for peer in (near, far, side, me_f)]

    def block(c, peer):
        return pl.ds(peer * share + c * per, per)

    groups = [(0, 1), (1, LINE), (LINE, 2 * LINE), (2 * LINE, chunks * LINE)]

    def request(group):
        for k in range(*groups[group]):
            here = block(*order[k])
            pltpu.make_async_copy(slopes.at[here], inputs.at[0, here], loads.at[group]).start()
            pltpu.make_async_copy(moments.at[here], inputs.at[1, here], loads.at[group]).start()

    request(0)
    fetch = pltpu.make_async_copy(weights, wbuf, loads.at[len(groups)])

    my_rows = pl.ds(pl.multiple_of(me_f * rows, rows), rows)

    def there(c, peer):
        return pltpu.make_async_remote_copy(
            src_ref=mom.at[block(c, peer)],
            dst_ref=xbuf.at[pl.ds(c * per, per), my_rows, :],
            send_sem=sends.at[0], recv_sem=frecv.at[c],
            device_id={"fsdp": peer}, device_id_type=MESH,
        )

    def gram_copy(c, d):
        return pltpu.make_async_remote_copy(
            src_ref=gsend.at[c, d - 1], dst_ref=grecv.at[c, d],
            send_sem=sends.at[2], recv_sem=gr.at[c],
            device_id={"tp": lax.rem(me_t + d, nt)}, device_id_type=MESH,
        )

    def factor_copy(c, d):
        return pltpu.make_async_remote_copy(
            src_ref=qrecv.at[c, 0], dst_ref=qrecv.at[c, d],
            send_sem=sends.at[3], recv_sem=qr.at[c],
            device_id={"tp": lax.rem(me_t + d, nt)}, device_id_type=MESH,
        )

    def grams(c):
        landed(out.at[pl.ds(0, (LINE - 1) * per)], frecv.at[c])
        for d in list(range(1, nt)) + [0]:
            first = c * per + lax.rem(me_t + d, nt) * each
            for e in range(each):
                x = xbuf[first + e]
                g = dot(x, x, ((1,), (1,)))
                if d == 0:
                    grecv[c, 0, e] = g
                else:
                    gsend[c, d - 1, e] = g
            if d > 0:
                gram_copy(c, d).start()

    def factors(c):
        landed(gsend.at[0], gr.at[c])
        for e in range(each):
            g = grecv[c, 0, e]
            for d in range(1, nt):
                g = g + grecv[c, d, e]
            qrecv[c, 0, e] = factor_of(g)
        for d in range(1, nt):
            factor_copy(c, d).start()

    def apply(c):
        for d in range(nt):
            if d == 1:
                landed(gsend.at[0], qr.at[c])
            first = c * per + lax.rem(me_t - d + nt, nt) * each
            for e in range(each):
                ybuf[first + e] = dot(qrecv[c, d, e], xbuf[first + e])

        def give(*cuts):
            for peer, cut in zip((far, near, side), cuts):
                for k, piece in enumerate(pieces[:cut]):
                    if piece[0] // per == c:
                        back_copy(ybuf, out, sends.at[1], brecv.at[k], share, me_f, peer, piece).start()

        each_job(pieces, give)
        own_rows(ybuf, out, share, me_f, (c * per, per))

    def momentum(group):
        first, last = groups[group]
        if last > first:
            landed(inputs.at[:, pl.ds(0, (last - first) * per)], loads.at[group])
        for k in range(first, last):
            c, peer = order[k]
            here = block(c, peer)
            value = hold_rate * inputs[1, here] + inputs[0, here]
            mom[here] = value
            if k % LINE == LINE - 1:
                xbuf[pl.ds(c * per, per), my_rows, :] = value

    momentum(0)
    request(1)

    @pl.when(inner)
    def _():
        pl.semaphore_wait(barrier, 1)
        there(0, near).start()
        tell(barrier, {"fsdp": side})

    request(2)
    request(3)
    fetch.start()
    for group in range(1, len(groups)):
        momentum(group)

    @pl.when(inner)
    def _():
        for c in range(1, min(chunks, AHEAD)):
            there(c, near).start()
        pl.semaphore_wait(hello, 2)
        tell(hello, {"fsdp": side})
        for c in range(chunks):
            for peer in (near, far, side) if c >= AHEAD else (far, side):
                there(c, peer).start()
        pl.semaphore_wait(ready, 1)

    @pl.when(outer)
    def _():
        pl.semaphore_wait(barrier, nt)
        tell(hello, {"fsdp": side})
        tell(hello, {"fsdp": near})
        for c in range(min(chunks, AHEAD)):
            for peer in (near, side):
                there(c, peer).start()
        pl.semaphore_wait(hello, 1)
        for c in range(chunks):
            for peer in (near, far, side) if c >= AHEAD else (far,):
                there(c, peer).start()
        tell_tp(ready)
        pl.semaphore_wait(ready, nt - 1)
        tell(ready, {"fsdp": side})

    for act, c in ORDER:
        (grams, factors, apply)[act](c)

    fetch.wait()

    def take(*cuts):
        for k, piece in enumerate(pieces[:cuts[-1]]):
            update(new, wbuf, out, brecv.at[k], share, piece)
        sent(out, sends.at[1], [pieces[:cut] for cut in cuts[:-1]])

    each_job(pieces, take)
    landed(mom.at[pl.ds(0, mats - share)], sends.at[0])
    landed(gsend, sends.at[2])
    landed(gsend, sends.at[3])


def last_kernel(chunks, ybuf, wbuf, written, new, out, sends, arrivals):
    me_f, far, near, side = places()
    share = ybuf.shape[0]
    pieces = pieces_of(share, chunks)
    barrier = pltpu.get_barrier_semaphore()

    def finish_job(*cuts):
        if min(cuts) == len(pieces):
            return
        for peer in (near, far, side):
            tell(barrier, {"fsdp": peer})
        pl.semaphore_wait(barrier, LINE - 1)
        for peer, cut in zip((far, near, side), cuts):
            for k, piece in list(enumerate(pieces))[cut:]:
                back_copy(ybuf, out, sends, arrivals.at[k], share, me_f, peer, piece).start()
        mine = list(enumerate(pieces))[cuts[-1]:]
        for _, piece in mine:
            own_rows(ybuf, out, share, me_f, piece)
        for k, piece in mine:
            update(new, wbuf, out, arrivals.at[k], share, piece)
        sent(out, sends, [pieces[cut:] for cut in cuts[:-1]])

    each_job(pieces, finish_job)


def copies_of(new, new_out, sems, share, pieces):
    copies = []
    for owner in range(LINE if pieces else 0):
        here = pl.ds(owner * share + pieces[0][0], sum(size for _, size in pieces))
        copies.append(pltpu.make_async_copy(new.at[here], new_out.at[here], sems.at[owner]))
    return copies


def write_first(chunks, new, mom, new_out, mom_out, sems):
    share = new.shape[0] // LINE
    pieces = pieces_of(share, chunks)

    def write(*cuts):
        copies = [pltpu.make_async_copy(mom, mom_out, sems.at[LINE])]
        copies += copies_of(new, new_out, sems, share, pieces[:cuts[-1]])
        for copy in copies:
            copy.start()
        for copy in copies:
            copy.wait()

    each_job(pieces, write)


def write_last(chunks, new, written, new_out, sems):
    share = new.shape[0] // LINE
    pieces = pieces_of(share, chunks)

    def write(*cuts):
        copies = copies_of(new, new_out, sems, share, pieces[cuts[-1]:])
        for copy in copies:
            copy.start()
        for copy in copies:
            copy.wait()

    each_job(pieces, write)


def stepped(nf, nt, slopes_in, moments_in, weights_in):
    mats, rows, wide = slopes_in.shape
    side, share = rows * nf, mats // nf
    chunks = CHUNKS
    per = share // chunks
    each = per // nt
    vmem, dma, flag = pltpu.VMEM, pltpu.SemaphoreType.DMA, pltpu.SemaphoreType.REGULAR
    shape = jax.ShapeDtypeStruct(slopes_in.shape, jnp.float32)
    whole = jax.ShapeDtypeStruct((share, side, wide), jnp.float32)
    held = [pl.BlockSpec(memory_space=pltpu.VMEM)]
    far = [pl.BlockSpec(memory_space=pltpu.HBM)]
    new, mom, results, weights = pl.pallas_call(
        functools.partial(kernel, nt, chunks),
        out_shape=[shape, shape, whole, shape],
        in_specs=far * 3,
        out_specs=held * 4,
        scratch_shapes=[
            vmem(slopes_in.shape, jnp.float32),
            vmem((2,) + slopes_in.shape, jnp.float32),
            vmem((share, side, wide), jnp.float32),
            vmem((chunks, nt - 1, each, side, side), jnp.float32),
            vmem((chunks, nt, each, side, side), jnp.float32),
            vmem((chunks, nt, each, side, side), jnp.float32),
            dma((4,)), dma((chunks,)), dma((chunks,)), dma((chunks,)), dma((chunks + 1,)),
            dma((5,)), flag, flag,
        ],
        compiler_params=pltpu.CompilerParams(
            collective_id=0, has_side_effects=True, vmem_limit_bytes=32 * 2**20
        ),
    )(*(pltpu.with_memory_space_constraint(x, pltpu.HBM) for x in (slopes_in, moments_in, weights_in)))
    new_out, mom_out = pl.pallas_call(
        functools.partial(write_first, chunks),
        out_shape=[shape] * 2,
        in_specs=held * 2,
        out_specs=far * 2,
        scratch_shapes=[dma((LINE + 1,))],
        compiler_params=pltpu.CompilerParams(vmem_limit_bytes=2**20),
    )(new, mom)
    new_out = pltpu.with_memory_space_constraint(new_out, pltpu.HBM)
    last = pl.pallas_call(
        functools.partial(last_kernel, chunks),
        out_shape=shape,
        in_specs=held * 2 + far,
        out_specs=held[0],
        scratch_shapes=[vmem(slopes_in.shape, jnp.float32), dma, dma((chunks + 1,))],
        compiler_params=pltpu.CompilerParams(
            collective_id=1, has_side_effects=True, vmem_limit_bytes=4 * 2**20
        ),
    )(results, weights, new_out)
    new_out = pl.pallas_call(
        functools.partial(write_last, chunks),
        out_shape=shape,
        in_specs=held + far,
        out_specs=far[0],
        input_output_aliases={1: 0},
        scratch_shapes=[dma((LINE,))],
        compiler_params=pltpu.CompilerParams(vmem_limit_bytes=2**20),
    )(last, new_out)
    return new_out, mom_out


def orthogonal_plain(new_momentum):
    moved = lax.all_to_all(new_momentum, "fsdp", split_axis=0, concat_axis=1, tiled=True)
    gram = lax.dot_general(moved, moved, (((2,), (2,)), ((0,), (0,))), precision=HIGHEST)
    gram = lax.psum_scatter(gram, "tp", scatter_dimension=0, tiled=True)
    factors = lax.all_gather(jax.vmap(factor_of)(gram), "tp", axis=0, tiled=True)
    whole = lax.dot_general(factors, moved, (((2,), (1,)), ((0,), (0,))), precision=HIGHEST)
    return lax.all_to_all(whole, "fsdp", split_axis=1, concat_axis=0, tiled=True)


def body(nf, nt, slopes_in, moments_in, weights_in):
    rows, wide = slopes_in.shape[1:]
    share = slopes_in.shape[0] // nf
    if nf == LINE and nt > 1 and share % (CHUNKS * nt) == 0 and share // CHUNKS > 1 and rows % 8 == 0 and wide % 128 == 0:
        return stepped(nf, nt, slopes_in, moments_in, weights_in)
    new_momentum = hold_rate * moments_in + slopes_in
    new_weights = weights_in - learn_rate * orthogonal_plain(new_momentum)
    return (new_weights, new_momentum)


def solution(mesh):
    placed = (P("job", "fsdp", "tp"), P("job", "fsdp", "tp"), P("job", "fsdp", "tp"))
    return jax.shard_map(
        functools.partial(body, mesh.shape["fsdp"], mesh.shape["tp"]),
        mesh=mesh,
        in_specs=placed,
        out_specs=(P("job", "fsdp", "tp"), P("job", "fsdp", "tp")),
        check_vma=False,
    )
```

```python
import functools

import jax
import jax.numpy as jnp
from jax import lax
from jax.experimental import pallas as pl
from jax.experimental.pallas import tpu as pltpu
from jax.sharding import PartitionSpec as P

ITERS = 5
LINE = 4
AHEAD = 2
LATE_PIECES = ((0, 0), (2, 2))
CHUNKS = 4
ORDER = ((0, 0), (1, 0), (2, 0), (0, 1), (1, 1), (0, 2), (2, 1), (1, 2), (0, 3), (1, 3), (2, 2), (2, 3))


hold_rate = 0.9
learn_rate = 0.8

COEF_A, COEF_B, COEF_C = 3.4445, -4.775, 2.0315
MESH = pl.DeviceIdType.MESH
HIGHEST = lax.Precision.HIGHEST


def dot(a, b, contract=((1,), (0,))):
    return lax.dot_general(
        a, b, (contract, ((), ())), precision=HIGHEST, preferred_element_type=jnp.float32
    )


def factor_of(gram):
    side = gram.shape[0]
    rows = lax.broadcasted_iota(jnp.int32, (side, side), 0)
    eye = rows == lax.broadcasted_iota(jnp.int32, (side, side), 1)
    total = jnp.sum(jnp.where(eye, gram, 0.0), axis=(0, 1), keepdims=True)
    scale = lax.rsqrt(total + 1e-06)

    def mixed_of(a):
        return COEF_B * a + COEF_C * dot(a, a)

    def step(_, carry):
        a, q = carry
        mixed = mixed_of(a)
        half = COEF_A * a + dot(mixed, a)
        return COEF_A * half + dot(half, mixed), COEF_A * q + dot(mixed, q)

    a = gram * scale * scale
    q = jnp.where(eye, jnp.broadcast_to(scale, gram.shape), 0.0)
    a, q = lax.fori_loop(0, ITERS - 1, step, (a, q))
    return COEF_A * q + dot(mixed_of(a), q)


def places():
    me_f = lax.axis_index("fsdp")
    half = me_f // 2
    return me_f, 3 - 3 * half, 2 - half, me_f + 1 - 2 * lax.rem(me_f, 2)


def tell(semaphore, device):
    pl.semaphore_signal(semaphore, inc=1, device_id=device, device_id_type=MESH)


def landed(ref, semaphore):
    pltpu.make_async_copy(ref, ref, semaphore).wait()


def pieces_of(share, chunks):
    per = share // chunks
    first = share - 2 * per
    whole = [(c * per, per) for c in range(chunks)]
    return whole[:-2] + [(first, per // 2), (first + per // 2, per - per // 2)] + whole[-1:]


def each_job(pieces, act):
    kind = lax.rem(lax.axis_index("job"), 2)
    me_f = lax.axis_index("fsdp")
    place = me_f * (3 - me_f)
    for number, late in enumerate(LATE_PIECES):
        ends, inside = (len(pieces) - few for few in late)
        if ends == inside:
            pl.when(kind == number)(functools.partial(act, ends, ends, ends, ends))
        else:
            pl.when((kind == number) & (place > 0))(functools.partial(act, ends, inside, ends, inside))
            pl.when((kind == number) & (place == 0))(functools.partial(act, ends, inside, inside, ends))


def back_copy(ybuf, out, sends, arrivals, share, me_f, peer, piece):
    start, size = piece
    rows = out.shape[1]
    theirs = pl.ds(pl.multiple_of(peer * rows, rows), rows)
    return pltpu.make_async_remote_copy(
        src_ref=ybuf.at[pl.ds(start, size), theirs, :],
        dst_ref=out.at[pl.ds(me_f * share + start, size)],
        send_sem=sends, recv_sem=arrivals,
        device_id={"fsdp": peer}, device_id_type=MESH,
    )


def own_rows(ybuf, out, share, me_f, piece):
    start, size = piece
    rows = out.shape[1]
    mine = pl.ds(pl.multiple_of(me_f * rows, rows), rows)
    out[pl.ds(me_f * share + start, size)] = ybuf[pl.ds(start, size), mine, :]


def update(new, wbuf, out, arrivals, share, piece):
    start, size = piece
    landed(out.at[pl.ds(0, (LINE - 1) * size)], arrivals)
    for owner in range(LINE):
        here = pl.ds(owner * share + start, size)
        new[here] = wbuf[here] - learn_rate * out[here]


def sent(out, sends, groups):
    total = sum(size for pieces in groups for _, size in pieces)
    landed(out.at[pl.ds(0, total)], sends)


def kernel(nt, chunks, slopes, moments, weights, new, mom, ybuf, wbuf, out, inputs, xbuf, gsend, grecv, qrecv, sends, frecv, gr, qr, brecv, loads, hello, ready):
    me_f, far, near, side = places()
    me_t = lax.axis_index("tp")
    mats, rows, _ = mom.shape
    share = mats // LINE
    per = share // chunks
    each = per // nt
    pieces = pieces_of(share, chunks)

    inner = me_f * (3 - me_f) > 0
    outer = me_f * (3 - me_f) == 0
    barrier = pltpu.get_barrier_semaphore()

    def tell_tp(semaphore):
        for d in range(1, nt):
            tell(semaphore, {"tp": lax.rem(me_t + d, nt)})

    @pl.when(inner)
    def _():
        tell(barrier, {"fsdp": near})

    @pl.when(outer)
    def _():
        tell_tp(barrier)

    order = [(c, peer) for c in range(chunks) for peer in (near, far, side, me_f)]

    def block(c, peer):
        return pl.ds(peer * share + c * per, per)

    groups = [(0, 1), (1, LINE), (LINE, 2 * LINE), (2 * LINE, chunks * LINE)]

    def request(group):
        for k in range(*groups[group]):
            here = block(*order[k])
            pltpu.make_async_copy(slopes.at[here], inputs.at[0, here], loads.at[group]).start()
            pltpu.make_async_copy(moments.at[here], inputs.at[1, here], loads.at[group]).start()

    request(0)
    fetch = pltpu.make_async_copy(weights, wbuf, loads.at[len(groups)])

    my_rows = pl.ds(pl.multiple_of(me_f * rows, rows), rows)

    def there(c, peer):
        return pltpu.make_async_remote_copy(
            src_ref=mom.at[block(c, peer)],
            dst_ref=xbuf.at[pl.ds(c * per, per), my_rows, :],
            send_sem=sends.at[0], recv_sem=frecv.at[c],
            device_id={"fsdp": peer}, device_id_type=MESH,
        )

    def gram_copy(c, d):
        return pltpu.make_async_remote_copy(
            src_ref=gsend.at[c, d - 1], dst_ref=grecv.at[c, d],
            send_sem=sends.at[2], recv_sem=gr.at[c],
            device_id={"tp": lax.rem(me_t + d, nt)}, device_id_type=MESH,
        )

    def factor_copy(c, d):
        return pltpu.make_async_remote_copy(
            src_ref=qrecv.at[c, 0], dst_ref=qrecv.at[c, d],
            send_sem=sends.at[3], recv_sem=qr.at[c],
            device_id={"tp": lax.rem(me_t + d, nt)}, device_id_type=MESH,
        )

    def grams(c):
        landed(out.at[pl.ds(0, (LINE - 1) * per)], frecv.at[c])
        for d in list(range(1, nt)) + [0]:
            first = c * per + lax.rem(me_t + d, nt) * each
            for e in range(each):
                x = xbuf[first + e]
                g = dot(x, x, ((1,), (1,)))
                if d == 0:
                    grecv[c, 0, e] = g
                else:
                    gsend[c, d - 1, e] = g
            if d > 0:
                gram_copy(c, d).start()

    def factors(c):
        landed(gsend.at[0], gr.at[c])
        for e in range(each):
            g = grecv[c, 0, e]
            for d in range(1, nt):
                g = g + grecv[c, d, e]
            qrecv[c, 0, e] = factor_of(g)
        for d in range(1, nt):
            factor_copy(c, d).start()

    def apply(c):
        for d in range(nt):
            if d == 1:
                landed(gsend.at[0], qr.at[c])
            first = c * per + lax.rem(me_t - d + nt, nt) * each
            for e in range(each):
                ybuf[first + e] = dot(qrecv[c, d, e], xbuf[first + e])

        def give(*cuts):
            for peer, cut in zip((far, near, side), cuts):
                for k, piece in enumerate(pieces[:cut]):
                    if piece[0] // per == c:
                        back_copy(ybuf, out, sends.at[1], brecv.at[k], share, me_f, peer, piece).start()

        each_job(pieces, give)
        own_rows(ybuf, out, share, me_f, (c * per, per))

    def momentum(group):
        first, last = groups[group]
        if last > first:
            landed(inputs.at[:, pl.ds(0, (last - first) * per)], loads.at[group])
        for k in range(first, last):
            c, peer = order[k]
            here = block(c, peer)
            value = hold_rate * inputs[1, here] + inputs[0, here]
            mom[here] = value
            if k % LINE == LINE - 1:
                xbuf[pl.ds(c * per, per), my_rows, :] = value

    momentum(0)
    request(1)

    @pl.when(inner)
    def _():
        pl.semaphore_wait(barrier, 1)
        there(0, near).start()
        tell(barrier, {"fsdp": side})

    request(2)
    request(3)
    fetch.start()
    for group in range(1, len(groups)):
        momentum(group)

    @pl.when(inner)
    def _():
        for c in range(1, min(chunks, AHEAD)):
            there(c, near).start()
        pl.semaphore_wait(hello, 2)
        tell(hello, {"fsdp": side})
        for c in range(chunks):
            for peer in (near, far, side) if c >= AHEAD else (far, side):
                there(c, peer).start()
        pl.semaphore_wait(ready, 1)

    @pl.when(outer)
    def _():
        pl.semaphore_wait(barrier, nt)
        tell(hello, {"fsdp": side})
        tell(hello, {"fsdp": near})
        for c in range(min(chunks, AHEAD)):
            for peer in (near, side):
                there(c, peer).start()
        pl.semaphore_wait(hello, 1)
        for c in range(chunks):
            for peer in (far, near, side) if c >= AHEAD else (far,):
                there(c, peer).start()
        tell_tp(ready)
        pl.semaphore_wait(ready, nt - 1)
        tell(ready, {"fsdp": side})

    for act, c in ORDER:
        (grams, factors, apply)[act](c)

    fetch.wait()

    def take(*cuts):
        for k, piece in enumerate(pieces[:cuts[-1]]):
            update(new, wbuf, out, brecv.at[k], share, piece)
        sent(out, sends.at[1], [pieces[:cut] for cut in cuts[:-1]])

    each_job(pieces, take)
    landed(mom.at[pl.ds(0, mats - share)], sends.at[0])
    landed(gsend, sends.at[2])
    landed(gsend, sends.at[3])


def last_kernel(chunks, ybuf, wbuf, written, new, out, sends, arrivals):
    me_f, far, near, side = places()
    share = ybuf.shape[0]
    pieces = pieces_of(share, chunks)
    barrier = pltpu.get_barrier_semaphore()

    def finish_job(*cuts):
        if min(cuts) == len(pieces):
            return
        for peer in (near, far, side):
            tell(barrier, {"fsdp": peer})
        pl.semaphore_wait(barrier, LINE - 1)
        for peer, cut in zip((far, near, side), cuts):
            for k, piece in list(enumerate(pieces))[cut:]:
                back_copy(ybuf, out, sends, arrivals.at[k], share, me_f, peer, piece).start()
        mine = list(enumerate(pieces))[cuts[-1]:]
        for _, piece in mine:
            own_rows(ybuf, out, share, me_f, piece)
        for k, piece in mine:
            update(new, wbuf, out, arrivals.at[k], share, piece)
        sent(out, sends, [pieces[cut:] for cut in cuts[:-1]])

    each_job(pieces, finish_job)


def copies_of(new, new_out, sems, share, pieces):
    copies = []
    for owner in range(LINE if pieces else 0):
        here = pl.ds(owner * share + pieces[0][0], sum(size for _, size in pieces))
        copies.append(pltpu.make_async_copy(new.at[here], new_out.at[here], sems.at[owner]))
    return copies


def write_first(chunks, new, mom, new_out, mom_out, sems):
    share = new.shape[0] // LINE
    pieces = pieces_of(share, chunks)

    def write(*cuts):
        copies = [pltpu.make_async_copy(mom, mom_out, sems.at[LINE])]
        copies += copies_of(new, new_out, sems, share, pieces[:cuts[-1]])
        for copy in copies:
            copy.start()
        for copy in copies:
            copy.wait()

    each_job(pieces, write)


def write_last(chunks, new, written, new_out, sems):
    share = new.shape[0] // LINE
    pieces = pieces_of(share, chunks)

    def write(*cuts):
        copies = copies_of(new, new_out, sems, share, pieces[cuts[-1]:])
        for copy in copies:
            copy.start()
        for copy in copies:
            copy.wait()

    each_job(pieces, write)


def stepped(nf, nt, slopes_in, moments_in, weights_in):
    mats, rows, wide = slopes_in.shape
    side, share = rows * nf, mats // nf
    chunks = CHUNKS
    per = share // chunks
    each = per // nt
    vmem, dma, flag = pltpu.VMEM, pltpu.SemaphoreType.DMA, pltpu.SemaphoreType.REGULAR
    shape = jax.ShapeDtypeStruct(slopes_in.shape, jnp.float32)
    whole = jax.ShapeDtypeStruct((share, side, wide), jnp.float32)
    held = [pl.BlockSpec(memory_space=pltpu.VMEM)]
    far = [pl.BlockSpec(memory_space=pltpu.HBM)]
    new, mom, results, weights = pl.pallas_call(
        functools.partial(kernel, nt, chunks),
        out_shape=[shape, shape, whole, shape],
        in_specs=far * 3,
        out_specs=held * 4,
        scratch_shapes=[
            vmem(slopes_in.shape, jnp.float32),
            vmem((2,) + slopes_in.shape, jnp.float32),
            vmem((share, side, wide), jnp.float32),
            vmem((chunks, nt - 1, each, side, side), jnp.float32),
            vmem((chunks, nt, each, side, side), jnp.float32),
            vmem((chunks, nt, each, side, side), jnp.float32),
            dma((4,)), dma((chunks,)), dma((chunks,)), dma((chunks,)), dma((chunks + 1,)),
            dma((5,)), flag, flag,
        ],
        compiler_params=pltpu.CompilerParams(
            collective_id=0, has_side_effects=True, vmem_limit_bytes=32 * 2**20
        ),
    )(*(pltpu.with_memory_space_constraint(x, pltpu.HBM) for x in (slopes_in, moments_in, weights_in)))
    new_out, mom_out = pl.pallas_call(
        functools.partial(write_first, chunks),
        out_shape=[shape] * 2,
        in_specs=held * 2,
        out_specs=far * 2,
        scratch_shapes=[dma((LINE + 1,))],
        compiler_params=pltpu.CompilerParams(vmem_limit_bytes=2**20),
    )(new, mom)
    new_out = pltpu.with_memory_space_constraint(new_out, pltpu.HBM)
    last = pl.pallas_call(
        functools.partial(last_kernel, chunks),
        out_shape=shape,
        in_specs=held * 2 + far,
        out_specs=held[0],
        scratch_shapes=[vmem(slopes_in.shape, jnp.float32), dma, dma((chunks + 1,))],
        compiler_params=pltpu.CompilerParams(
            collective_id=1, has_side_effects=True, vmem_limit_bytes=4 * 2**20
        ),
    )(results, weights, new_out)
    new_out = pl.pallas_call(
        functools.partial(write_last, chunks),
        out_shape=shape,
        in_specs=held + far,
        out_specs=far[0],
        input_output_aliases={1: 0},
        scratch_shapes=[dma((LINE,))],
        compiler_params=pltpu.CompilerParams(vmem_limit_bytes=2**20),
    )(last, new_out)
    return new_out, mom_out


def orthogonal_plain(new_momentum):
    moved = lax.all_to_all(new_momentum, "fsdp", split_axis=0, concat_axis=1, tiled=True)
    gram = lax.dot_general(moved, moved, (((2,), (2,)), ((0,), (0,))), precision=HIGHEST)
    gram = lax.psum_scatter(gram, "tp", scatter_dimension=0, tiled=True)
    factors = lax.all_gather(jax.vmap(factor_of)(gram), "tp", axis=0, tiled=True)
    whole = lax.dot_general(factors, moved, (((2,), (1,)), ((0,), (0,))), precision=HIGHEST)
    return lax.all_to_all(whole, "fsdp", split_axis=1, concat_axis=0, tiled=True)


def body(nf, nt, slopes_in, moments_in, weights_in):
    rows, wide = slopes_in.shape[1:]
    share = slopes_in.shape[0] // nf
    if nf == LINE and nt > 1 and share % (CHUNKS * nt) == 0 and share // CHUNKS > 1 and rows % 8 == 0 and wide % 128 == 0:
        return stepped(nf, nt, slopes_in, moments_in, weights_in)
    new_momentum = hold_rate * moments_in + slopes_in
    new_weights = weights_in - learn_rate * orthogonal_plain(new_momentum)
    return (new_weights, new_momentum)


def solution(mesh):
    placed = (P("job", "fsdp", "tp"), P("job", "fsdp", "tp"), P("job", "fsdp", "tp"))
    return jax.shard_map(
        functools.partial(body, mesh.shape["fsdp"], mesh.shape["tp"]),
        mesh=mesh,
        in_specs=placed,
        out_specs=(P("job", "fsdp", "tp"), P("job", "fsdp", "tp")),
        check_vma=False,
    )
```
